32 devices in a mesh: cluster: 8 (over z, x), sub: 4 (over y, core).
Axes of the slice: x: 2, y: 2, z: 4, core: 2. Of those that a mesh axis runs over, the one named last changes fastest.
Arguments:
- mantissas: int32 [8, 64, 168, 128], P('cluster', 'sub'), may hold values from -128 to 127
- exponents: int32 [8, 64, 14], P('cluster', 'sub'), may hold values from -9 to -6
- channel: bfloat16 [8, 64, 2, 64, 128], P('cluster', 'sub'), may hold values from -0.5 to 0.5
- inverses: bfloat16 [8, 64, 2, 128, 128], P('cluster', 'sub'), may hold values from -4 to 4, as said below
Outputs:
- detected: bfloat16 [64, 168, 256], P('sub')
The draws below stay inside these ranges and needn't reach their ends.
Inputs may be any that keep to these rules, and one draw needn't show every extreme that they name: `inverses`: each real part has a positive diagonal; the matrices are otherwise dense.
All inputs are finite; a program needn't handle non-finite values.
Results may differ from the reference program's by a relative error of at most 0.0074.
Values may be sent and summed in bfloat16 or wider, within the bound.
A program may use at most 64 MiB of HBM per device.

```python
import jax
import jax.numpy as jnp
from jax import lax

USER_COUNT = 128
CLUSTER_ANTENNAS = 64
BLOCK_TONES = 12
SLOT_SYMBOLS = 14
ITERS = 3
RESOURCE_BLOCKS = 64
ANTENNA_GROUPS = 8


def draw_inverses(key, part):
    first, second = jax.random.split(key, 2)
    shape = (ANTENNA_GROUPS, RESOURCE_BLOCKS, 2, USER_COUNT, USER_COUNT)
    noise = jax.random.normal(first, shape, jnp.float32) * 0.05
    diagonal = jax.random.uniform(second, (ANTENNA_GROUPS, RESOURCE_BLOCKS, 1, USER_COUNT, 1), jnp.float32, 0.5, 1.5)
    identity = jnp.eye(USER_COUNT, dtype=jnp.float32)
    realpart = (jnp.arange(2) == 0).astype(jnp.float32)[None, None, :, None, None]
    result = noise + diagonal * identity * realpart
    return result.astype(jnp.bfloat16)


def with_ends(drawn, rng, least, high):
    extent = drawn.shape
    spot = [jax.random.randint(jax.random.fold_in(rng, axis), (), 0, extent[axis]) for axis in range(len(extent))]
    drawn = drawn.at[tuple(spot)].set(least)
    longest = extent.index(max(extent))
    spot[longest] = (spot[longest] + 1) % extent[longest]
    return drawn.at[tuple(spot)].set(high)


def level_of(stream_key, extent, shards, least, largest):
    gain, own = 1.0, jax.random.fold_in(stream_key, 6)
    for position, blocks in shards:
        draws = jnp.exp(jax.random.uniform(jax.random.fold_in(own, position), (blocks,), jnp.float32, least / len(shards), largest / len(shards)))
        gain = gain * jnp.repeat(draws, extent[position] // blocks).reshape([-1 if axis == position else 1 for axis in range(len(extent))])
    return gain


def scatter_about(rng, dims, deviation, reach, cuts=(), held_as=jnp.bfloat16):
    values = deviation * jax.random.normal(rng, dims, jnp.float32)
    if cuts:
        values = values * level_of(rng, dims, cuts, -0.22, 0.18)
    return jnp.clip(values, -reach, reach).astype(held_as)


def setup_inputs(seed: int = 0) -> dict:
    splits = jax.random.split(jax.random.key(seed), 5)
    mantissas = with_ends(jax.random.randint(splits[0], (ANTENNA_GROUPS, RESOURCE_BLOCKS, SLOT_SYMBOLS * BLOCK_TONES, 2 * CLUSTER_ANTENNAS), -128, 128), jax.random.fold_in(splits[0], 1), -128, 127).astype(jnp.int32)
    exponents = with_ends(jax.random.randint(splits[1], (ANTENNA_GROUPS, RESOURCE_BLOCKS, SLOT_SYMBOLS), -9, -5), jax.random.fold_in(splits[1], 1), -9, (-5) - 1).astype(jnp.int32)
    channel = scatter_about(splits[2], (ANTENNA_GROUPS, RESOURCE_BLOCKS, 2, CLUSTER_ANTENNAS, USER_COUNT), (2 * CLUSTER_ANTENNAS) ** -0.5, 0.5, ((0, 8), (1, 4)))
    inverses = draw_inverses(jax.random.fold_in(splits[4], 71), 0)
    return dict(mantissas=mantissas, exponents=exponents, channel=channel, inverses=inverses)


RHO = 0.5

def complex_block(real, imag):
    top = jnp.concatenate([real, -imag], axis=-1)
    bottom = jnp.concatenate([imag, real], axis=-1)
    return jnp.concatenate([top, bottom], axis=-2)

def one_block(index, mantissas, exponents, channel, inverses):
    mant = lax.dynamic_index_in_dim(mantissas, index, 1, keepdims=False)
    expo = lax.dynamic_index_in_dim(exponents, index, 1, keepdims=False)
    chan = lax.dynamic_index_in_dim(channel, index, 1, keepdims=False)
    inv = lax.dynamic_index_in_dim(inverses, index, 1, keepdims=False)
    scale = jnp.repeat(jnp.exp2(expo.astype(jnp.float32)), BLOCK_TONES, axis=1)
    signal = (mant.astype(jnp.float32) * scale[:, :, None]).astype(jnp.bfloat16)
    match = complex_block(chan[:, 0], chan[:, 1])
    matched_filter = jnp.einsum('csa,cau->csu', signal.astype(jnp.float32), match.astype(jnp.float32))
    solve_block = complex_block(inv[:, 0], inv[:, 1]).astype(jnp.float32)
    consensus = jnp.zeros(matched_filter.shape[1:], jnp.float32)
    dual = jnp.zeros(matched_filter.shape, jnp.float32)
    for step in range(ITERS):
        rhs = (matched_filter + RHO * (consensus[None] - dual)).astype(jnp.bfloat16)
        local = jnp.einsum('csk,cjk->csj', rhs.astype(jnp.float32), solve_block)
        term = local + dual
        total = lax.optimization_barrier(jnp.sum(term, axis=0))
        consensus = (total / ANTENNA_GROUPS).astype(jnp.bfloat16).astype(jnp.float32)
        dual = term - consensus[None]
    return consensus.astype(jnp.bfloat16)

def reference(mantissas, exponents, channel, inverses):

    def per_block(index):
        return one_block(index, mantissas, exponents, channel, inverses)
    consensus = lax.map(per_block, jnp.arange(RESOURCE_BLOCKS, dtype=jnp.int32)).astype(jnp.float32)
    column_list = lax.optimization_barrier(jnp.sum(consensus * consensus, axis=(0, 1)))
    power = (column_list[:USER_COUNT] + column_list[USER_COUNT:]) / (RESOURCE_BLOCKS * SLOT_SYMBOLS * BLOCK_TONES)
    factor = lax.rsqrt(power + 1e-06)
    factor = jnp.concatenate([factor, factor])
    return (consensus * factor).astype(jnp.bfloat16)
```

```python
import functools

import jax
import jax.numpy as jnp
from jax import lax
from jax.experimental import pallas as pl
from jax.experimental.pallas import tpu as pltpu
from jax.sharding import PartitionSpec as P

ITERS = 3


RHO = 0.5
MESH = pl.DeviceIdType.MESH


def complex_block(real, imag):
    top = jnp.concatenate([real, -imag], axis=-1)
    bottom = jnp.concatenate([imag, real], axis=-1)
    return jnp.concatenate([top, bottom], axis=-2)


def reduce_plan(mantissas, exponents, channel, inverses):
    clusters = lax.axis_size("cluster")
    mant = mantissas[0]
    blocks, vectors, _ = mant.shape
    expo = exponents[0]
    scale = jnp.repeat(jnp.exp2(expo.astype(jnp.float32)), vectors // expo.shape[1], axis=1)
    signal = (mant.astype(jnp.float32) * scale[:, :, None]).astype(jnp.bfloat16)
    match = complex_block(channel[0, :, 0], channel[0, :, 1])
    matched_filter = jnp.einsum("rsa,rau->rsu", signal, match, preferred_element_type=jnp.float32)
    solve_block = complex_block(inverses[0, :, 0], inverses[0, :, 1])
    width = matched_filter.shape[2]
    consensus = jnp.zeros(matched_filter.shape, jnp.float32)
    dual = jnp.zeros(matched_filter.shape, jnp.float32)
    for step in range(ITERS):
        rhs = (matched_filter + RHO * (consensus - dual)).astype(jnp.bfloat16)
        local = jnp.einsum("rsk,rjk->rsj", rhs, solve_block, preferred_element_type=jnp.float32)
        term = local + dual
        flat = term.reshape(blocks * vectors, width)
        share = lax.psum_scatter(flat, "cluster", scatter_dimension=0, tiled=True)
        average = (share / clusters).astype(jnp.bfloat16)
        gathered = lax.all_gather(average, "cluster", axis=0, tiled=True)
        consensus = gathered.reshape(blocks, vectors, width).astype(jnp.float32)
        dual = term - consensus
    users = width // 2
    column_list = jnp.sum(consensus * consensus, axis=(0, 1))
    partial_value = column_list[:users] + column_list[users:]
    total_power = lax.psum(partial_value, "sub")
    power = total_power / (blocks * lax.axis_size("sub") * vectors)
    factor = lax.rsqrt(power + 1e-06)
    factor = jnp.concatenate([factor, factor])
    return (consensus * factor).astype(jnp.bfloat16)


def kernel(
    n, subs,
    mant_hbm, expo_ref, chan_hbm, inv_hbm,
    out_ref, factor_ref,
    mant_v, sig_v, r_sig, r_chan, r_inv, match_v, solve_v, matched_v, term_v, cons_v, power_v, r_pow, r_sub,
    local_sem, own_sem, send_sem, recv_sem, ag_send, ag_recv, fw_send, fw_recv, pw_send, pw_recv, sb_send, sb_recv,
):
    me = lax.axis_index("cluster")
    my_sub = lax.axis_index("sub")
    blocks, vectors, ants = mant_v.shape
    per = blocks // n
    symbols = expo_ref.shape[2]
    tones = vectors // symbols
    half = ants // 2
    users = chan_hbm.shape[4]
    width = 2 * users
    partner = me + 1 - 2 * lax.rem(me, 2)

    def peer(off):
        return lax.rem(me + off, n)

    def source(off):
        return lax.rem(me + n - off, n)

    def remote(src, dst, send, recv, where):
        return pltpu.make_async_remote_copy(
            src_ref=src, dst_ref=dst, send_sem=send, recv_sem=recv, device_id=where, device_id_type=MESH
        )

    def deal(kind, off, b):
        index = peer(off) * per + b
        src, dst = (
            (inv_hbm.at[0, index], r_inv.at[off, b]),
            (chan_hbm.at[0, index], r_chan.at[off, b]),
            (sig_v.at[index], r_sig.at[off, b]),
        )[kind]
        return remote(src, dst, send_sem.at[kind, off, b], recv_sem.at[kind, off, b], {"cluster": peer(off)})

    def own(kind, b):
        index = me * per + b
        src, dst = (
            (inv_hbm.at[0, index], r_inv.at[0, b]),
            (chan_hbm.at[0, index], r_chan.at[0, b]),
        )[kind]
        return pltpu.make_async_copy(src, dst, own_sem.at[kind, b])

    def gather(off, b):
        slot = out_ref.at[me * per + b]
        return remote(slot, slot, ag_send.at[off, b], ag_recv.at[off, b], {"cluster": peer(off)})

    def gather_partner(b):
        slot = out_ref.at[me * per + b]
        return remote(slot, slot, ag_send.at[0, b], ag_recv.at[0, b], {"cluster": partner})

    def forward(off, b):
        slot = out_ref.at[source(off) * per + b]
        return remote(slot, slot, fw_send.at[off, b], fw_recv.at[off, b], {"cluster": partner})

    def share_power(off):
        slot = r_pow.at[me]
        return remote(slot, slot, pw_send.at[off], pw_recv.at[off], {"cluster": peer(off)})

    def share_sub(off):
        slot = r_sub.at[my_sub]
        return remote(slot, slot, sb_send.at[off], sb_recv.at[off], {"sub": lax.rem(my_sub + off, subs)})

    load = pltpu.make_async_copy(mant_hbm.at[0], mant_v, local_sem)
    load.start()
    for b in range(per):
        own(0, b).start()
        own(1, b).start()
    barrier = pltpu.get_barrier_semaphore()
    for off in range(1, n):
        pl.semaphore_signal(barrier, inc=1, device_id={"cluster": peer(off)}, device_id_type=MESH)
    for off in range(1, subs):
        pl.semaphore_signal(
            barrier, inc=1, device_id={"sub": lax.rem(my_sub + off, subs)}, device_id_type=MESH
        )
    pl.semaphore_wait(barrier, n - 1 + subs - 1)

    for off in range(1, n):
        deal(1, off, 0).start()
        deal(0, off, 0).start()
    row = lax.broadcasted_iota(jnp.int32, (vectors, symbols), 0)
    first = lax.broadcasted_iota(jnp.int32, (vectors, symbols), 1) * tones
    spread = jnp.where((row >= first) & (row < first + tones), 1.0, 0.0).astype(jnp.bfloat16)
    steps = jnp.exp2(expo_ref[0].astype(jnp.float32)).astype(jnp.bfloat16)
    scale = lax.dot_general(spread, steps, (((1,), (1,)), ((), ())), preferred_element_type=jnp.float32)
    load.wait()
    for b in range(per):
        for p in range(n):
            g = p * per + b
            sig_v[g] = (mant_v[g].astype(jnp.float32) * scale[:, g : g + 1]).astype(jnp.bfloat16)
        for off in range(1, n):
            if b > 0:
                deal(1, off, b).start()
                deal(0, off, b).start()
            deal(2, off, b).start()
    power_v[...] = jnp.zeros_like(power_v)

    def solve(rhs, off):
        return lax.dot_general(
            rhs.astype(jnp.bfloat16), solve_v[off], (((1,), (1,)), ((), ())), preferred_element_type=jnp.float32
        )

    def one_slot(b, carry):
        total = None
        for off in range(n):
            if off == 0:
                own(0, b).wait()
                own(1, b).wait()
                signal = sig_v[me * per + b]
            else:
                for kind in range(3):
                    deal(kind, off, b).wait_recv()
                signal = r_sig[off, b]
            real, imag = r_chan[off, b, 0], r_chan[off, b, 1]
            match_v[off, :half, :users] = real
            match_v[off, :half, users:] = -imag
            match_v[off, half:, :users] = imag
            match_v[off, half:, users:] = real
            real, imag = r_inv[off, b, 0], r_inv[off, b, 1]
            solve_v[off, :users, :users] = real
            solve_v[off, :users, users:] = -imag
            solve_v[off, users:, :users] = imag
            solve_v[off, users:, users:] = real
            matched = jnp.dot(signal, match_v[off], preferred_element_type=jnp.float32)
            matched_v[off] = matched
            term = solve(matched, off)
            term_v[off] = term
            total = term if total is None else total + term
        for step in range(1, ITERS):
            cons_v[...] = (total / n).astype(jnp.bfloat16).astype(jnp.float32)
            total = None
            for off in range(n):
                consensus = cons_v[...]
                dual = term_v[off] - consensus
                term = solve(matched_v[off] + RHO * (consensus - dual), off) + dual
                if step < ITERS - 1:
                    term_v[off] = term
                total = term if total is None else total + term
        final = (total / n).astype(jnp.bfloat16)
        out_ref[me * per + b] = final
        final = final.astype(jnp.float32)
        columns = jnp.sum(final * final, axis=0, keepdims=True)
        power_v[...] += columns[:, :users] + columns[:, users:]
        for off in range(2, n, 2):
            gather(off, b).start()
        gather_partner(b).start()
        return carry

    lax.fori_loop(0, per, one_slot, 0)

    r_pow[me] = power_v[...]
    for off in range(1, n):
        share_power(off).start()
    for off in range(1, n):
        share_power(off).wait_recv()
    r_sub[my_sub] = jnp.sum(r_pow[...], axis=0)
    for off in range(1, subs):
        share_sub(off).start()
    for b in range(per):
        for off in range(2, n, 2):
            gather(off, b).wait_recv()
            forward(off, b).start()
    for off in range(1, subs):
        share_sub(off).wait_recv()
    power = jnp.sum(r_sub[...], axis=0) / (blocks * subs * vectors)
    factor = lax.rsqrt(power + 1e-06)
    factor_ref[:, :users] = factor
    factor_ref[:, users:] = factor
    for b in range(per):
        for off in range(1, n):
            for kind in range(3):
                deal(kind, off, b).wait_send()
        gather_partner(b).wait()
        for off in range(2, n, 2):
            gather(off, b).wait_send()
            forward(off, b).wait()
    for off in range(1, n):
        share_power(off).wait_send()
    for off in range(1, subs):
        share_sub(off).wait_send()


def regroup_plan(n, subs, mantissas, exponents, channel, inverses):
    _, blocks, vectors, ants = mantissas.shape
    users = channel.shape[4]
    width = 2 * users
    per = blocks // n
    flops = 2 * blocks * vectors * width * (ants + ITERS * width)
    dma = pltpu.SemaphoreType.DMA
    consensus, factor = pl.pallas_call(
        functools.partial(kernel, n, subs),
        out_shape=(
            jax.ShapeDtypeStruct((blocks, vectors, width), jnp.bfloat16),
            jax.ShapeDtypeStruct((1, width), jnp.float32),
        ),
        in_specs=[
            pl.BlockSpec(memory_space=pl.ANY),
            pl.BlockSpec(memory_space=pltpu.VMEM),
            pl.BlockSpec(memory_space=pl.ANY),
            pl.BlockSpec(memory_space=pl.ANY),
        ],
        out_specs=(
            pl.BlockSpec(memory_space=pltpu.VMEM),
            pl.BlockSpec(memory_space=pltpu.VMEM),
        ),
        scratch_shapes=[
            pltpu.VMEM((blocks, vectors, ants), jnp.int32),
            pltpu.VMEM((blocks, vectors, ants), jnp.bfloat16),
            pltpu.VMEM((n, per, vectors, ants), jnp.bfloat16),
            pltpu.VMEM((n, per) + channel.shape[2:], jnp.bfloat16),
            pltpu.VMEM((n, per) + inverses.shape[2:], jnp.bfloat16),
            pltpu.VMEM((n, ants, width), jnp.bfloat16),
            pltpu.VMEM((n, width, width), jnp.bfloat16),
            pltpu.VMEM((n, vectors, width), jnp.float32),
            pltpu.VMEM((n, vectors, width), jnp.float32),
            pltpu.VMEM((vectors, width), jnp.float32),
            pltpu.VMEM((1, users), jnp.float32),
            pltpu.VMEM((n, 1, users), jnp.float32),
            pltpu.VMEM((subs, 1, users), jnp.float32),
            dma,
            dma((2, per)),
            dma((3, n, per)),
            dma((3, n, per)),
            dma((n, per)),
            dma((n, per)),
            dma((n, per)),
            dma((n, per)),
            dma((n,)),
            dma((n,)),
            dma((subs,)),
            dma((subs,)),
        ],
        compiler_params=pltpu.CompilerParams(
            collective_id=0, has_side_effects=True, vmem_limit_bytes=48 * 1024 * 1024
        ),
        cost_estimate=pl.CostEstimate(flops=flops, bytes_accessed=8 * blocks * vectors * width, transcendentals=0),
    )(mantissas, exponents, channel, inverses)
    return (consensus.astype(jnp.float32) * factor[None]).astype(jnp.bfloat16)


def solution(mesh):
    n, subs = mesh.shape["cluster"], mesh.shape["sub"]

    def per_device(mantissas, exponents, channel, inverses):
        blocks = mantissas.shape[1]
        if n % 2 == 0 and blocks % n == 0:
            return regroup_plan(n, subs, mantissas, exponents, channel, inverses)
        return reduce_plan(mantissas, exponents, channel, inverses)

    placed = (
        P("cluster", "sub", None, None),
        P("cluster", "sub", None),
        P("cluster", "sub", None, None, None),
        P("cluster", "sub", None, None, None),
    )
    return jax.shard_map(
        per_device, mesh=mesh, in_specs=placed, out_specs=P("sub", None, None), check_vma=False
    )
```

```python
import functools

import jax
import jax.numpy as jnp
from jax import lax
from jax.experimental import pallas as pl
from jax.experimental.pallas import tpu as pltpu
from jax.sharding import PartitionSpec as P

ITERS = 3


RHO = 0.5
MESH = pl.DeviceIdType.MESH


def complex_block(real, imag):
    top = jnp.concatenate([real, -imag], axis=-1)
    bottom = jnp.concatenate([imag, real], axis=-1)
    return jnp.concatenate([top, bottom], axis=-2)


def reduce_plan(mantissas, exponents, channel, inverses):
    clusters = lax.axis_size("cluster")
    mant = mantissas[0]
    blocks, vectors, _ = mant.shape
    expo = exponents[0]
    scale = jnp.repeat(jnp.exp2(expo.astype(jnp.float32)), vectors // expo.shape[1], axis=1)
    signal = (mant.astype(jnp.float32) * scale[:, :, None]).astype(jnp.bfloat16)
    match = complex_block(channel[0, :, 0], channel[0, :, 1])
    matched_filter = jnp.einsum("rsa,rau->rsu", signal, match, preferred_element_type=jnp.float32)
    solve_block = complex_block(inverses[0, :, 0], inverses[0, :, 1])
    width = matched_filter.shape[2]
    consensus = jnp.zeros(matched_filter.shape, jnp.float32)
    dual = jnp.zeros(matched_filter.shape, jnp.float32)
    for step in range(ITERS):
        rhs = (matched_filter + RHO * (consensus - dual)).astype(jnp.bfloat16)
        local = jnp.einsum("rsk,rjk->rsj", rhs, solve_block, preferred_element_type=jnp.float32)
        term = local + dual
        flat = term.reshape(blocks * vectors, width)
        share = lax.psum_scatter(flat, "cluster", scatter_dimension=0, tiled=True)
        average = (share / clusters).astype(jnp.bfloat16)
        gathered = lax.all_gather(average, "cluster", axis=0, tiled=True)
        consensus = gathered.reshape(blocks, vectors, width).astype(jnp.float32)
        dual = term - consensus
    users = width // 2
    column_list = jnp.sum(consensus * consensus, axis=(0, 1))
    partial_value = column_list[:users] + column_list[users:]
    total_power = lax.psum(partial_value, "sub")
    power = total_power / (blocks * lax.axis_size("sub") * vectors)
    factor = lax.rsqrt(power + 1e-06)
    factor = jnp.concatenate([factor, factor])
    return (consensus * factor).astype(jnp.bfloat16)


def lowest_bit(mask):
    bit = 0
    while not (mask >> bit) & 1:
        bit += 1
    return bit


def row_parts(vectors):
    cut = min(vectors, -(-vectors // 32) * 16)
    return [(0, cut)] + ([(cut, vectors - cut)] if cut < vectors else [])


def kernel(
    n, subs,
    mant_hbm, expo_ref, chan_hbm, inv_hbm,
    out_ref, factor_ref,
    mant_v, sig_v, r_sig, r_chan, r_inv, match_v, solve_v, matched_v, term_v, cons_v, power_v, r_pow, r_sub,
    local_sem, own_sem, send_sem, recv_sem, ag_send, ag_recv, pw_send, pw_recv, sb_send, sb_recv,
):
    me = lax.axis_index("cluster")
    my_sub = lax.axis_index("sub")
    blocks, vectors, ants = mant_v.shape
    per = blocks // n
    symbols = expo_ref.shape[2]
    tones = vectors // symbols
    half = ants // 2
    users = chan_hbm.shape[4]
    bits = n.bit_length() - 1
    parts = row_parts(vectors)

    def flip(mask):
        index = me
        for bit in range(bits):
            if (mask >> bit) & 1:
                index = index + (1 - 2 * lax.rem(me // 2**bit, 2)) * 2**bit
        return index

    def remote(src, dst, send, recv, where):
        return pltpu.make_async_remote_copy(
            src_ref=src, dst_ref=dst, send_sem=send, recv_sem=recv, device_id=where, device_id_type=MESH
        )

    def deal(kind, mask, b):
        index = flip(mask) * per + b
        if kind == 0:
            src, dst = inv_hbm.at[0, index], r_inv.at[mask, b]
        elif kind == 1:
            src, dst = chan_hbm.at[0, index], r_chan.at[mask, b]
        else:
            rows = pl.ds(*parts[kind - 2])
            src, dst = sig_v.at[index, rows], r_sig.at[mask, b, rows]
        return remote(src, dst, send_sem.at[kind, mask, b], recv_sem.at[kind, mask, b], {"cluster": flip(mask)})

    def own(kind, b):
        index = me * per + b
        src, dst = (
            (inv_hbm.at[0, index], r_inv.at[0, b]),
            (chan_hbm.at[0, index], r_chan.at[0, b]),
        )[kind]
        return pltpu.make_async_copy(src, dst, own_sem.at[kind, b])

    def gather(mask, b, part):
        bit = lowest_bit(mask)
        slot = out_ref.at[flip(mask - 2**bit) * per + b, pl.ds(*parts[part])]
        return remote(
            slot, slot, ag_send.at[part, mask, b], ag_recv.at[part, mask, b], {"cluster": flip(2**bit)}
        )

    def pass_on(masks, b, part):
        for mask in masks:
            gather(mask, b, part).wait_recv()
            for bit in reversed(range(lowest_bit(mask))):
                gather(mask + 2**bit, b, part).start()

    relayed = [mask for mask in range(1, n) if mask % 2 == 0]
    early = [mask for mask in relayed if mask == 2 ** lowest_bit(mask)][::-1]
    late = sorted((mask for mask in relayed if mask not in early), key=lambda m: (bin(m).count("1"), -m))
    final = [mask for mask in range(1, n) if mask % 2]

    def share_power(mask):
        slot = r_pow.at[me]
        return remote(slot, slot, pw_send.at[mask], pw_recv.at[mask], {"cluster": flip(mask)})

    def share_sub(off):
        slot = r_sub.at[my_sub]
        return remote(slot, slot, sb_send.at[off], sb_recv.at[off], {"sub": lax.rem(my_sub + off, subs)})

    load = pltpu.make_async_copy(mant_hbm.at[0], mant_v, local_sem)
    load.start()
    for b in range(per):
        own(0, b).start()
        own(1, b).start()
    barrier = pltpu.get_barrier_semaphore()
    for mask in range(1, n):
        pl.semaphore_signal(barrier, inc=1, device_id={"cluster": flip(mask)}, device_id_type=MESH)
    for off in range(1, subs):
        pl.semaphore_signal(
            barrier, inc=1, device_id={"sub": lax.rem(my_sub + off, subs)}, device_id_type=MESH
        )
    pl.semaphore_wait(barrier, n - 1 + subs - 1)

    order = [mask for bit in reversed(range(bits)) for mask in range(2**bit, 2 ** (bit + 1))]
    for mask in order:
        deal(1, mask, 0).start()
        deal(0, mask, 0).start()
    row = lax.broadcasted_iota(jnp.int32, (vectors, symbols), 0)
    first = lax.broadcasted_iota(jnp.int32, (vectors, symbols), 1) * tones
    spread = jnp.where((row >= first) & (row < first + tones), 1.0, 0.0).astype(jnp.bfloat16)
    steps = jnp.exp2(expo_ref[0].astype(jnp.float32)).astype(jnp.bfloat16)
    scale = lax.dot_general(spread, steps, (((1,), (1,)), ((), ())), preferred_element_type=jnp.float32)
    load.wait()
    for b in range(per):
        for p in range(n):
            g = p * per + b
            sig_v[g] = (mant_v[g].astype(jnp.float32) * scale[:, g : g + 1]).astype(jnp.bfloat16)
        if b > 0:
            for mask in order:
                deal(1, mask, b).start()
                deal(0, mask, b).start()
        for part in range(len(parts)):
            for mask in order:
                deal(2 + part, mask, b).start()
    power_v[...] = jnp.zeros_like(power_v)

    def solve(rhs, c):
        return lax.dot_general(
            rhs.astype(jnp.bfloat16), solve_v[c], (((1,), (1,)), ((), ())), preferred_element_type=jnp.float32
        )

    def one_slot(b, carry):
        for part, (at, count) in enumerate(parts):
            rows = pl.ds(at, count)
            total = None
            for c in [0] + order[::-1]:
                if part == 0:
                    if c == 0:
                        own(0, b).wait()
                        own(1, b).wait()
                    else:
                        deal(1, c, b).wait_recv()
                        deal(0, c, b).wait_recv()
                    real, imag = r_chan[c, b, 0], r_chan[c, b, 1]
                    match_v[c, :half, :users] = real
                    match_v[c, :half, users:] = -imag
                    match_v[c, half:, :users] = imag
                    match_v[c, half:, users:] = real
                    real, imag = r_inv[c, b, 0], r_inv[c, b, 1]
                    solve_v[c, :users, :users] = real
                    solve_v[c, :users, users:] = -imag
                    solve_v[c, users:, :users] = imag
                    solve_v[c, users:, users:] = real
                if c == 0:
                    signal = sig_v[me * per + b, rows]
                else:
                    deal(2 + part, c, b).wait_recv()
                    signal = r_sig[c, b, rows]
                matched = jnp.dot(signal, match_v[c], preferred_element_type=jnp.float32)
                matched_v[c, rows] = matched
                term = solve(matched, c)
                term_v[c, rows] = term
                total = term if total is None else total + term

            @pl.when(b > 0)
            def _():
                pass_on(early, b - 1, part)

            for step in range(1, ITERS):
                cons_v[rows] = (total / n).astype(jnp.bfloat16).astype(jnp.float32)
                total = None
                for c in range(n):
                    consensus = cons_v[rows]
                    dual = term_v[c, rows] - consensus
                    term = solve(matched_v[c, rows] + RHO * (consensus - dual), c) + dual
                    if step < ITERS - 1:
                        term_v[c, rows] = term
                    total = term if total is None else total + term
            done = (total / n).astype(jnp.bfloat16)
            out_ref[me * per + b, rows] = done
            for bit in reversed(range(bits)):
                gather(2**bit, b, part).start()
            done = done.astype(jnp.float32)
            columns = jnp.sum(done * done, axis=0, keepdims=True)
            power_v[...] += columns[:, :users] + columns[:, users:]

            @pl.when(b > 0)
            def _():
                pass_on(late, b - 1, part)

        return carry

    lax.fori_loop(0, per, one_slot, 0)

    r_pow[me] = power_v[...]
    for mask in range(1, n):
        share_power(mask).start()
    last = per - 1
    for part in range(len(parts)):
        pass_on(early, last, part)
    for mask in range(1, n):
        share_power(mask).wait_recv()
    r_sub[my_sub] = jnp.sum(r_pow[...], axis=0)
    for off in range(1, subs):
        share_sub(off).start()
    for part in range(len(parts)):
        pass_on(late, last, part)
    for off in range(1, subs):
        share_sub(off).wait_recv()
    power = jnp.sum(r_sub[...], axis=0) / (blocks * subs * vectors)
    factor = lax.rsqrt(power + 1e-06)
    factor_ref[:, :users] = factor
    factor_ref[:, users:] = factor
    for b in range(per):
        for mask in range(1, n):
            for kind in range(2 + len(parts)):
                deal(kind, mask, b).wait_send()
            for part in range(len(parts)):
                gather(mask, b, part).wait_send()
        for mask in final:
            for part in range(len(parts)):
                gather(mask, b, part).wait_recv()
    for mask in range(1, n):
        share_power(mask).wait_send()
    for off in range(1, subs):
        share_sub(off).wait_send()


def regroup_plan(n, subs, mantissas, exponents, channel, inverses):
    _, blocks, vectors, ants = mantissas.shape
    users = channel.shape[4]
    width = 2 * users
    per = blocks // n
    parts = len(row_parts(vectors))
    flops = 2 * blocks * vectors * width * (ants + ITERS * width)
    dma = pltpu.SemaphoreType.DMA
    consensus, factor = pl.pallas_call(
        functools.partial(kernel, n, subs),
        out_shape=(
            jax.ShapeDtypeStruct((blocks, vectors, width), jnp.bfloat16),
            jax.ShapeDtypeStruct((1, width), jnp.float32),
        ),
        in_specs=[
            pl.BlockSpec(memory_space=pl.ANY),
            pl.BlockSpec(memory_space=pltpu.VMEM),
            pl.BlockSpec(memory_space=pl.ANY),
            pl.BlockSpec(memory_space=pl.ANY),
        ],
        out_specs=(
            pl.BlockSpec(memory_space=pltpu.VMEM),
            pl.BlockSpec(memory_space=pltpu.VMEM),
        ),
        scratch_shapes=[
            pltpu.VMEM((blocks, vectors, ants), jnp.int32),
            pltpu.VMEM((blocks, vectors, ants), jnp.bfloat16),
            pltpu.VMEM((n, per, vectors, ants), jnp.bfloat16),
            pltpu.VMEM((n, per) + channel.shape[2:], jnp.bfloat16),
            pltpu.VMEM((n, per) + inverses.shape[2:], jnp.bfloat16),
            pltpu.VMEM((n, ants, width), jnp.bfloat16),
            pltpu.VMEM((n, width, width), jnp.bfloat16),
            pltpu.VMEM((n, vectors, width), jnp.float32),
            pltpu.VMEM((n, vectors, width), jnp.float32),
            pltpu.VMEM((vectors, width), jnp.float32),
            pltpu.VMEM((1, users), jnp.float32),
            pltpu.VMEM((n, 1, users), jnp.float32),
            pltpu.VMEM((subs, 1, users), jnp.float32),
            dma,
            dma((2, per)),
            dma((2 + parts, n, per)),
            dma((2 + parts, n, per)),
            dma((parts, n, per)),
            dma((parts, n, per)),
            dma((n,)),
            dma((n,)),
            dma((subs,)),
            dma((subs,)),
        ],
        compiler_params=pltpu.CompilerParams(
            collective_id=0, has_side_effects=True, vmem_limit_bytes=60 * 1024 * 1024
        ),
        cost_estimate=pl.CostEstimate(flops=flops, bytes_accessed=8 * blocks * vectors * width, transcendentals=0),
    )(mantissas, exponents, channel, inverses)
    return (consensus.astype(jnp.float32) * factor[None]).astype(jnp.bfloat16)


def solution(mesh):
    n, subs = mesh.shape["cluster"], mesh.shape["sub"]

    def per_device(mantissas, exponents, channel, inverses):
        blocks = mantissas.shape[1]
        if n > 1 and n & (n - 1) == 0 and blocks % n == 0:
            return regroup_plan(n, subs, mantissas, exponents, channel, inverses)
        return reduce_plan(mantissas, exponents, channel, inverses)

    placed = (
        P("cluster", "sub", None, None),
        P("cluster", "sub", None),
        P("cluster", "sub", None, None, None),
        P("cluster", "sub", None, None, None),
    )
    return jax.shard_map(
        per_device, mesh=mesh, in_specs=placed, out_specs=P("sub", None, None), check_vma=False
    )
```

```python
import functools

import jax
import jax.numpy as jnp
from jax import lax
from jax.experimental import pallas as pl
from jax.experimental.pallas import tpu as pltpu
from jax.sharding import PartitionSpec as P

ITERS = 3


RHO = 0.5
MESH = pl.DeviceIdType.MESH


def complex_block(real, imag):
    top = jnp.concatenate([real, -imag], axis=-1)
    bottom = jnp.concatenate([imag, real], axis=-1)
    return jnp.concatenate([top, bottom], axis=-2)


def reduce_plan(mantissas, exponents, channel, inverses):
    clusters = lax.axis_size("cluster")
    mant = mantissas[0]
    blocks, vectors, _ = mant.shape
    expo = exponents[0]
    scale = jnp.repeat(jnp.exp2(expo.astype(jnp.float32)), vectors // expo.shape[1], axis=1)
    signal = (mant.astype(jnp.float32) * scale[:, :, None]).astype(jnp.bfloat16)
    match = complex_block(channel[0, :, 0], channel[0, :, 1])
    matched_filter = jnp.einsum("rsa,rau->rsu", signal, match, preferred_element_type=jnp.float32)
    solve_block = complex_block(inverses[0, :, 0], inverses[0, :, 1])
    width = matched_filter.shape[2]
    consensus = jnp.zeros(matched_filter.shape, jnp.float32)
    dual = jnp.zeros(matched_filter.shape, jnp.float32)
    for step in range(ITERS):
        rhs = (matched_filter + RHO * (consensus - dual)).astype(jnp.bfloat16)
        local = jnp.einsum("rsk,rjk->rsj", rhs, solve_block, preferred_element_type=jnp.float32)
        term = local + dual
        flat = term.reshape(blocks * vectors, width)
        share = lax.psum_scatter(flat, "cluster", scatter_dimension=0, tiled=True)
        average = (share / clusters).astype(jnp.bfloat16)
        gathered = lax.all_gather(average, "cluster", axis=0, tiled=True)
        consensus = gathered.reshape(blocks, vectors, width).astype(jnp.float32)
        dual = term - consensus
    users = width // 2
    column_list = jnp.sum(consensus * consensus, axis=(0, 1))
    partial_value = column_list[:users] + column_list[users:]
    total_power = lax.psum(partial_value, "sub")
    power = total_power / (blocks * lax.axis_size("sub") * vectors)
    factor = lax.rsqrt(power + 1e-06)
    factor = jnp.concatenate([factor, factor])
    return (consensus * factor).astype(jnp.bfloat16)


def lowest_bit(mask):
    bit = 0
    while not (mask >> bit) & 1:
        bit += 1
    return bit


def row_parts(vectors):
    cut = min(vectors, -(-vectors // 32) * 16)
    return [(0, cut)] + ([(cut, vectors - cut)] if cut < vectors else [])


def kernel(
    n, subs,
    mant_hbm, expo_ref, chan_hbm, inv_hbm,
    out_ref, factor_ref,
    mant_v, sig_v, r_sig, r_chan, r_inv, match_v, solve_v, matched_v, term_v, cons_v, power_v, r_pow, r_sub,
    local_sem, own_sem, send_sem, recv_sem, ag_send, ag_recv, pw_send, pw_recv, sb_send, sb_recv,
):
    me = lax.axis_index("cluster")
    my_sub = lax.axis_index("sub")
    blocks, vectors, ants = mant_v.shape
    per = blocks // n
    symbols = expo_ref.shape[2]
    tones = vectors // symbols
    half = ants // 2
    users = chan_hbm.shape[4]
    bits = n.bit_length() - 1
    parts = row_parts(vectors)

    def flip(mask):
        index = me
        for bit in range(bits):
            if (mask >> bit) & 1:
                index = index + (1 - 2 * lax.rem(me // 2**bit, 2)) * 2**bit
        return index

    def remote(src, dst, send, recv, where):
        return pltpu.make_async_remote_copy(
            src_ref=src, dst_ref=dst, send_sem=send, recv_sem=recv, device_id=where, device_id_type=MESH
        )

    def deal(kind, mask, b):
        index = flip(mask) * per + b
        if kind == 0:
            src, dst = inv_hbm.at[0, index], r_inv.at[mask, b]
        elif kind == 1:
            src, dst = chan_hbm.at[0, index], r_chan.at[mask, b]
        else:
            rows = pl.ds(*parts[kind - 2])
            src, dst = sig_v.at[index, rows], r_sig.at[mask, b, rows]
        return remote(src, dst, send_sem.at[kind, mask, b], recv_sem.at[kind, mask, b], {"cluster": flip(mask)})

    def own(kind, b):
        index = me * per + b
        src, dst = (
            (inv_hbm.at[0, index], r_inv.at[0, b]),
            (chan_hbm.at[0, index], r_chan.at[0, b]),
        )[kind]
        return pltpu.make_async_copy(src, dst, own_sem.at[kind, b])

    def gather(mask, b, part):
        bit = lowest_bit(mask)
        slot = out_ref.at[flip(mask - 2**bit) * per + b, pl.ds(*parts[part])]
        return remote(
            slot, slot, ag_send.at[part, mask, b], ag_recv.at[part, mask, b], {"cluster": flip(2**bit)}
        )

    def pass_on(masks, b, part):
        for mask in masks:
            gather(mask, b, part).wait_recv()
            for bit in reversed(range(lowest_bit(mask))):
                gather(mask + 2**bit, b, part).start()

    relayed = [mask for mask in range(1, n) if mask % 2 == 0]
    early = [mask for mask in relayed if mask == 2 ** lowest_bit(mask)][::-1]
    late = sorted((mask for mask in relayed if mask not in early), key=lambda m: (bin(m).count("1"), -m))
    final = [mask for mask in range(1, n) if mask % 2]

    def share_power(mask):
        slot = r_pow.at[me]
        return remote(slot, slot, pw_send.at[mask], pw_recv.at[mask], {"cluster": flip(mask)})

    def share_sub(off):
        slot = r_sub.at[my_sub]
        return remote(slot, slot, sb_send.at[off], sb_recv.at[off], {"sub": lax.rem(my_sub + off, subs)})

    load = pltpu.make_async_copy(mant_hbm.at[0], mant_v, local_sem)
    load.start()
    for b in range(per):
        own(0, b).start()
        own(1, b).start()
    barrier = pltpu.get_barrier_semaphore()
    for mask in range(1, n):
        pl.semaphore_signal(barrier, inc=1, device_id={"cluster": flip(mask)}, device_id_type=MESH)
    for off in range(1, subs):
        pl.semaphore_signal(
            barrier, inc=1, device_id={"sub": lax.rem(my_sub + off, subs)}, device_id_type=MESH
        )
    pl.semaphore_wait(barrier, n - 1 + subs - 1)

    order = [mask for bit in reversed(range(bits)) for mask in range(2**bit, 2 ** (bit + 1))]
    for mask in order:
        deal(1, mask, 0).start()
        deal(0, mask, 0).start()
    row = lax.broadcasted_iota(jnp.int32, (vectors, symbols), 0)
    first = lax.broadcasted_iota(jnp.int32, (vectors, symbols), 1) * tones
    spread = jnp.where((row >= first) & (row < first + tones), 1.0, 0.0).astype(jnp.bfloat16)
    steps = jnp.exp2(expo_ref[0].astype(jnp.float32)).astype(jnp.bfloat16)
    scale = lax.dot_general(spread, steps, (((1,), (1,)), ((), ())), preferred_element_type=jnp.float32)
    load.wait()
    for b in range(per):
        for p in range(n):
            g = p * per + b
            sig_v[g] = (mant_v[g].astype(jnp.float32) * scale[:, g : g + 1]).astype(jnp.bfloat16)
        if b > 0:
            for mask in order:
                deal(1, mask, b).start()
                deal(0, mask, b).start()
        for part in range(len(parts)):
            for mask in order:
                deal(2 + part, mask, b).start()
    power_v[...] = jnp.zeros_like(power_v)

    def solve(rhs, c):
        return lax.dot_general(
            rhs.astype(jnp.bfloat16), solve_v[c], (((1,), (1,)), ((), ())), preferred_element_type=jnp.float32
        )

    def relay(masks, b, part):
        if part > 0:
            pass_on(masks, b, part - 1)
        else:

            @pl.when(b > 0)
            def _():
                pass_on(masks, b - 1, len(parts) - 1)

    def one_slot(b, carry):
        for part, (at, count) in enumerate(parts):
            rows = pl.ds(at, count)
            total = None
            for c in [0] + order[::-1]:
                if part == 0:
                    if c == 0:
                        own(0, b).wait()
                        own(1, b).wait()
                    else:
                        deal(1, c, b).wait_recv()
                        deal(0, c, b).wait_recv()
                    real, imag = r_chan[c, b, 0], r_chan[c, b, 1]
                    match_v[c, :half, :users] = real
                    match_v[c, :half, users:] = -imag
                    match_v[c, half:, :users] = imag
                    match_v[c, half:, users:] = real
                    real, imag = r_inv[c, b, 0], r_inv[c, b, 1]
                    solve_v[c, :users, :users] = real
                    solve_v[c, :users, users:] = -imag
                    solve_v[c, users:, :users] = imag
                    solve_v[c, users:, users:] = real
                if c == 0:
                    signal = sig_v[me * per + b, rows]
                else:
                    deal(2 + part, c, b).wait_recv()
                    signal = r_sig[c, b, rows]
                matched = jnp.dot(signal, match_v[c], preferred_element_type=jnp.float32)
                matched_v[c, rows] = matched
                term = solve(matched, c)
                term_v[c, rows] = term
                total = term if total is None else total + term

            for step in range(1, ITERS):
                if step == ITERS - 1:
                    relay(early, b, part)
                cons_v[rows] = (total / n).astype(jnp.bfloat16).astype(jnp.float32)
                total = None
                for c in range(n):
                    consensus = cons_v[rows]
                    dual = term_v[c, rows] - consensus
                    term = solve(matched_v[c, rows] + RHO * (consensus - dual), c) + dual
                    if step < ITERS - 1:
                        term_v[c, rows] = term
                    total = term if total is None else total + term
            done = (total / n).astype(jnp.bfloat16)
            out_ref[me * per + b, rows] = done
            done = done.astype(jnp.float32)
            columns = jnp.sum(done * done, axis=0, keepdims=True)
            power_v[...] += columns[:, :users] + columns[:, users:]
            if part == len(parts) - 1:

                @pl.when(b == per - 1)
                def _():
                    r_pow[me] = power_v[...]
                    for mask in order:
                        share_power(mask).start()

            for bit in reversed(range(bits)):
                gather(2**bit, b, part).start()
            relay(late, b, part)

        return carry

    lax.fori_loop(0, per, one_slot, 0)

    last = per - 1
    pass_on(early, last, len(parts) - 1)
    for mask in range(1, n):
        share_power(mask).wait_recv()
    r_sub[my_sub] = jnp.sum(r_pow[...], axis=0)
    for off in range(1, subs):
        share_sub(off).start()
    pass_on(late, last, len(parts) - 1)
    for off in range(1, subs):
        share_sub(off).wait_recv()
    power = jnp.sum(r_sub[...], axis=0) / (blocks * subs * vectors)
    factor = lax.rsqrt(power + 1e-06)
    factor_ref[:, :users] = factor
    factor_ref[:, users:] = factor
    for b in range(per):
        for mask in range(1, n):
            for kind in range(2 + len(parts)):
                deal(kind, mask, b).wait_send()
            for part in range(len(parts)):
                gather(mask, b, part).wait_send()
        for mask in final:
            for part in range(len(parts)):
                gather(mask, b, part).wait_recv()
    for mask in range(1, n):
        share_power(mask).wait_send()
    for off in range(1, subs):
        share_sub(off).wait_send()


def regroup_plan(n, subs, mantissas, exponents, channel, inverses):
    _, blocks, vectors, ants = mantissas.shape
    users = channel.shape[4]
    width = 2 * users
    per = blocks // n
    parts = len(row_parts(vectors))
    flops = 2 * blocks * vectors * width * (ants + ITERS * width)
    dma = pltpu.SemaphoreType.DMA
    consensus, factor = pl.pallas_call(
        functools.partial(kernel, n, subs),
        out_shape=(
            jax.ShapeDtypeStruct((blocks, vectors, width), jnp.bfloat16),
            jax.ShapeDtypeStruct((1, width), jnp.float32),
        ),
        in_specs=[
            pl.BlockSpec(memory_space=pltpu.HBM),
            pl.BlockSpec(memory_space=pltpu.VMEM),
            pl.BlockSpec(memory_space=pltpu.HBM),
            pl.BlockSpec(memory_space=pltpu.HBM),
        ],
        out_specs=(
            pl.BlockSpec(memory_space=pltpu.VMEM),
            pl.BlockSpec(memory_space=pltpu.VMEM),
        ),
        scratch_shapes=[
            pltpu.VMEM((blocks, vectors, ants), jnp.int32),
            pltpu.VMEM((blocks, vectors, ants), jnp.bfloat16),
            pltpu.VMEM((n, per, vectors, ants), jnp.bfloat16),
            pltpu.VMEM((n, per) + channel.shape[2:], jnp.bfloat16),
            pltpu.VMEM((n, per) + inverses.shape[2:], jnp.bfloat16),
            pltpu.VMEM((n, ants, width), jnp.bfloat16),
            pltpu.VMEM((n, width, width), jnp.bfloat16),
            pltpu.VMEM((n, vectors, width), jnp.float32),
            pltpu.VMEM((n, vectors, width), jnp.float32),
            pltpu.VMEM((vectors, width), jnp.float32),
            pltpu.VMEM((1, users), jnp.float32),
            pltpu.VMEM((n, 1, users), jnp.float32),
            pltpu.VMEM((subs, 1, users), jnp.float32),
            dma,
            dma((2, per)),
            dma((2 + parts, n, per)),
            dma((2 + parts, n, per)),
            dma((parts, n, per)),
            dma((parts, n, per)),
            dma((n,)),
            dma((n,)),
            dma((subs,)),
            dma((subs,)),
        ],
        compiler_params=pltpu.CompilerParams(
            collective_id=0, has_side_effects=True, vmem_limit_bytes=60 * 1024 * 1024
        ),
        cost_estimate=pl.CostEstimate(flops=flops, bytes_accessed=8 * blocks * vectors * width, transcendentals=0),
    )(mantissas, exponents, channel, inverses)
    return (consensus.astype(jnp.float32) * factor[None]).astype(jnp.bfloat16)


def solution(mesh):
    n, subs = mesh.shape["cluster"], mesh.shape["sub"]

    def per_device(mantissas, exponents, channel, inverses):
        blocks = mantissas.shape[1]
        if n > 1 and n & (n - 1) == 0 and blocks % n == 0:
            return regroup_plan(n, subs, mantissas, exponents, channel, inverses)
        return reduce_plan(mantissas, exponents, channel, inverses)

    placed = (
        P("cluster", "sub", None, None),
        P("cluster", "sub", None),
        P("cluster", "sub", None, None, None),
        P("cluster", "sub", None, None, None),
    )
    return jax.shard_map(
        per_device, mesh=mesh, in_specs=placed, out_specs=P("sub", None, None), check_vma=False
    )
```
